32 devices in a mesh: scen: 2 (over y), cell: 4 (over z), obs: 4 (over x, core).
Axes of the slice: x: 2, y: 2, z: 4, core: 2. Of those that a mesh axis runs over, the one named last changes fastest.
Arguments:
- prior: bfloat16 [400, 2048], P('scen', 'cell'), parts along dimension 0, may hold values from -6 to 6
- obs_block: int32 [4096], P('obs'), may hold values from 0 to 15
- obs_weight: bfloat16 [4096, 128], P('obs'), may hold values from -0.5 to 0.5
- observed: float32 [8192], P(('scen', 'obs')), parts along dimension 0, may hold values from -8 to 8
- obs_sigma: float32 [4096], P('obs'), may hold values from 0.5 to 1.5
- pert_seed: int32 [6, 200, 4096], P('scen', None, 'obs'), parts along dimension 0, may hold values from 0 to 1048575
Outputs:
- posterior: bfloat16 [400, 2048], P('scen', 'cell'), parts along dimension 0
- post_predicted: float32 [400, 4096], P('scen', 'obs'), parts along dimension 0
The draws below stay inside these ranges and needn't reach their ends.
There are 2 independent parts, one for each index of `scen`. The reference program is written for one: setup_inputs(seed, part) draws one part's arguments, and reference() takes and returns one part's arrays. A program takes and returns all parts, laid end to end along the dimension named above; an argument that names none is the same for every part. Nothing has to cross between parts.
All inputs are finite; a program needn't handle non-finite values.
Results may differ from the reference program's by a relative error of at most 0.0013.
Values sent between devices are 32-bit elements; how exact they have to be, the bound alone decides.
A program may use at most 64 MiB of HBM per device.

```python
import math
import jax
import jax.numpy as jnp
from jax import lax

E = 200
NOBS = 4096
BLK = 128
ITERS = 3
NCELL = 2048
NBLK = 16


def set_ends(drawn, own_key, low, high):
    longest = drawn.shape.index(max(drawn.shape))
    spots = []
    for shift in (0, 1):
        where = [jax.random.randint(jax.random.fold_in(own_key, axis), (), 0, length) for axis, length in enumerate(drawn.shape)]
        where[longest] = (where[longest] + shift) % drawn.shape[longest]
        spots.append(tuple(where))
    return drawn.at[spots[0]].set(low).at[spots[1]].set(high)


def steps_of(own_key, dims, cuts, low, top_value):
    def one(dim, parts):
        draws = jax.random.uniform(jax.random.fold_in(jax.random.fold_in(own_key, 6), dim), (parts,), jnp.float32, low / len(cuts), top_value / len(cuts))
        return jnp.repeat(jnp.exp(draws), dims[dim] // parts).reshape((-1,) + (1,) * (len(dims) - dim - 1))

    level = one(*cuts[0])
    for cut in cuts[1:]:
        level = level * one(*cut)
    return level


def centred(stream_key, extent, spread, most, pieces=(), kind=jnp.bfloat16):
    loudness = steps_of(stream_key, extent, pieces, -0.22, 0.18) if pieces else 1.0
    values = jax.random.normal(stream_key, extent, jnp.float32) * spread * loudness
    return jnp.minimum(jnp.maximum(values, -most), most).astype(kind)


def setup_inputs(seed: int = 0, part: int = 0) -> dict:
    key_list = jax.random.split(jax.random.key(seed), 7)
    part_keys = jax.random.split(jax.random.fold_in(key_list[6], part), 7)
    return {
        "prior": centred(part_keys[0], (E, NCELL), 1.0, 6.0, ((1, 4),)),
        "obs_block": set_ends(jax.random.randint(key_list[1], (NOBS,), 0, NBLK), jax.random.fold_in(key_list[1], 1), 0, NBLK - 1).astype(jnp.int32),
        "obs_weight": centred(key_list[2], (NOBS, BLK), BLK ** -0.5, 0.5, ((0, 4),)),
        "observed": centred(part_keys[3], (NOBS,), 1.5, 8.0, ((0, 4),), jnp.float32),
        "obs_sigma": jnp.clip(jnp.exp(math.log(1.5) - 1.0986123 * jax.random.uniform(key_list[4], (NOBS,), jnp.float32) ** steps_of(key_list[4], (NOBS,), ((0, 4),), -0.2, 0.2)), 0.5, 1.5),
        "pert_seed": set_ends(jax.random.randint(part_keys[5], (ITERS, E, NOBS), 0, 1048576), jax.random.fold_in(part_keys[5], 1), 0, 1048575).astype(jnp.int32),
    }


def apply_operator(param_field, obs_block, obs_weight):
    blocks = param_field.reshape(E, NBLK, BLK)
    groups = NOBS // 64
    indices = obs_block.reshape(groups, 64)
    weights = obs_weight.astype(jnp.float32).reshape(groups, 64, BLK)

    def one_group(operands):
        group_index, group_weight = operands
        picked = jnp.take(blocks, group_index, axis=1)
        return lax.optimization_barrier(jnp.sum(picked * group_weight[None], axis=2))
    result = lax.map(one_group, (indices, weights))
    return jnp.transpose(result, (1, 0, 2)).reshape(E, NOBS)

def reference(prior, obs_block, obs_weight, observed, obs_sigma, pert_seed):
    param_field = prior.astype(jnp.float32)
    inflation = jnp.float32(ITERS)
    hp = lax.Precision.HIGHEST
    for step_index in range(ITERS):
        predicted = apply_operator(param_field, obs_block, obs_weight)
        noise = jnp.sqrt(jnp.float32(3.0)) * ((2.0 * pert_seed[step_index].astype(jnp.float32) + 1.0) / 1048576.0 - 1.0)
        misfit = observed[None, :] + jnp.sqrt(inflation) * obs_sigma[None, :] * noise - predicted
        dev_pred = predicted - lax.optimization_barrier(jnp.mean(predicted, axis=0, keepdims=True))
        dev_field = param_field - lax.optimization_barrier(jnp.mean(param_field, axis=0, keepdims=True))
        cov = jnp.dot(dev_pred.T, dev_pred, precision=hp) / (E - 1.0)
        system = cov + jnp.diag(inflation * obs_sigma * obs_sigma)
        solved = jnp.linalg.solve(system, misfit.T)
        member_weight = jnp.dot(dev_pred, solved, precision=hp)
        param_field = param_field + jnp.dot(member_weight.T, dev_field, precision=hp) / (E - 1.0)
    post_predicted = apply_operator(param_field, obs_block, obs_weight)
    return (param_field.astype(jnp.bfloat16), post_predicted)
```

```python
import functools

import jax
import jax.numpy as jnp
from jax import lax
from jax.experimental import pallas as pl
from jax.experimental.pallas import tpu as pltpu
from jax.sharding import PartitionSpec as P

BLK = 128
ITERS = 3
MESH = pl.DeviceIdType.MESH
VM = pl.BlockSpec(memory_space=pltpu.VMEM)
NN = (((1,), (0,)), ((), ()))
NT = (((1,), (1,)), ((), ()))


def mm(a, b, dims):
    return lax.dot_general(a, b, dims, preferred_element_type=jnp.float32)


def split(x):
    hi = x.astype(jnp.bfloat16)
    return hi, (x - hi.astype(jnp.float32)).astype(jnp.bfloat16)


def dot3(a, b, dims):
    ah, al = split(a)
    bh, bl = split(b)
    return mm(ah, bh, dims) + (mm(ah, bl, dims) + mm(al, bh, dims))


def dot_exact(a, b, dims):
    return lax.dot_general(a, b, dims, precision=lax.Precision.HIGHEST, preferred_element_type=jnp.float32)


def block_predictions(fields, weights, block):
    total = None
    for field, first in fields:
        for b in range(field.shape[1] // BLK):
            part = mm(field[:, b * BLK:(b + 1) * BLK].astype(jnp.bfloat16), weights[...], NT)
            here = block == first + b
            total = jnp.where(here, part, 0.0 if total is None else total)
    return total


def sums_kernel(n_cell, n_obs, prior, block, weights, observed, sigma, seeds, out, acc, fin, obs_recv, cell_recv,
                send_sem, recv_sem):
    members, width = prior.shape
    cell, obs = lax.axis_index("cell"), lax.axis_index("obs")
    bits = [1 << k for k in range(n_obs.bit_length() - 1)]
    barrier = pltpu.get_barrier_semaphore()
    for bit in bits:
        pl.semaphore_signal(barrier, inc=1, device_id={"obs": obs ^ bit}, device_id_type=MESH)
    for d in range(1, n_cell):
        pl.semaphore_signal(barrier, inc=1, device_id={"cell": lax.rem(cell + d, n_cell)}, device_id_type=MESH)

    nblocks = width // BLK
    first = cell * nblocks
    blk = block[...]
    predicted = block_predictions([(prior, first)], weights, blk)
    inside = jnp.logical_and(blk >= first, blk < first + nblocks)
    mean = jnp.mean(predicted, axis=0, keepdims=True)
    inv = 1.0 / sigma[...]
    dev = (predicted - mean) * jnp.where(inside, inv, 0.0)
    base = (observed[...] - mean) * inv + (3.0 / 1048576.0 - 3.0)
    ah, al = split(dev)
    scale = 1.0 / (members - 1.0)
    rows = acc.shape[1]

    def noisy(i):
        return split(base + seeds[i].astype(jnp.float32) * (6.0 / 1048576.0))

    def put(s, k, h, l):
        acc[s, k * members:(k + 1) * members, 0:members] = (
            mm(h, ah, NT) + (mm(h, al, NT) + mm(l, ah, NT))) * scale

    acc[...] = jnp.zeros_like(acc)

    nbit = len(bits)
    lens = [rows >> k for k in range(nbit + 1)]
    offs = [jnp.int32(0)]
    for k in range(nbit):
        offs.append(pl.multiple_of(offs[-1] + ((obs >> k) & 1) * lens[k + 1], 8))
    quarter, off = lens[-1], offs[-1]
    chunk = quarter // n_cell
    stages = 2 * nbit + 2
    obs_at = [0]
    for k in range(nbit):
        obs_at.append(obs_at[-1] + lens[k + 1])

    def copies(s, stage):
        made = []
        if stage < nbit:
            n = lens[stage + 1]
            src = pl.multiple_of(offs[stage] + (1 - ((obs >> stage) & 1)) * n, 8)
            made.append((acc.at[s, pl.ds(src, n)], obs_recv.at[s, pl.ds(obs_at[stage], n)], {"obs": obs ^ bits[stage]}))
        elif stage == nbit:
            for d in range(1, n_cell):
                to = lax.rem(cell + d, n_cell)
                src = pl.multiple_of(off + to * chunk, 8)
                made.append((acc.at[s, pl.ds(src, chunk)], cell_recv.at[s, d - 1], {"cell": to}))
        elif stage == nbit + 1:
            src = pl.multiple_of(off + cell * chunk, 8)
            for d in range(1, n_cell):
                to = lax.rem(cell + d, n_cell)
                made.append((fin.at[s, pl.ds(src, chunk)], fin.at[s, pl.ds(src, chunk)], {"cell": to}))
        else:
            k = stages - 1 - stage
            n = lens[k + 1]
            made.append((fin.at[s, pl.ds(offs[k + 1], n)], fin.at[s, pl.ds(offs[k + 1], n)], {"obs": obs ^ bits[k]}))
        return [
            pltpu.make_async_remote_copy(src_ref=a, dst_ref=b, send_sem=send_sem.at[s, stage, j],
                                         recv_sem=recv_sem.at[s, stage, j], device_id=to, device_id_type=MESH)
            for j, (a, b, to) in enumerate(made)
        ]

    flights = {}

    def start(s, stage):
        flights[s, stage] = copies(s, stage)
        for c in flights[s, stage]:
            c.start()

    def finish(s, stage):
        for c in flights[s, stage]:
            c.wait()
        if stage < nbit:
            n = lens[stage + 1]
            mine = pl.ds(offs[stage + 1], n)
            acc[s, mine] = acc[s, mine] + obs_recv[s, pl.ds(obs_at[stage], n)]
        elif stage == nbit:
            mine = pl.ds(pl.multiple_of(off + cell * chunk, 8), chunk)
            total = acc[s, mine]
            for d in range(1, n_cell):
                total = total + cell_recv[s, d - 1]
            fin[s, mine] = total

    put(0, 0, ah, al)
    put(0, 1, *noisy(0))
    pl.semaphore_wait(barrier, len(bits) + n_cell - 1)
    start(0, 0)
    put(1, 0, *noisy(1))
    put(1, 1, *noisy(2))
    for stage in range(stages + 1):
        if stage < stages:
            finish(0, stage)
            if stage + 1 < stages:
                start(0, stage + 1)
        if stage > 0:
            finish(1, stage - 1)
        if stage < stages:
            start(1, stage)
    for s in range(2):
        for k in range(2):
            out[2 * s + k] = fin[s, k * members:(k + 1) * members, 0:members]


def solve_kernel(sums, result, stack, dev_op):
    members = result.shape[0]
    row = lax.broadcasted_iota(jnp.int32, (members, members), 0)
    col = lax.broadcasted_iota(jnp.int32, (members, members), 1)
    eye = jnp.where(row == col, 1.0, 0.0)
    inflation = float(ITERS)
    up, down = pl.ds(0, members), pl.ds(members, members)

    def solve(gram, cross):
        system = gram + inflation * eye
        bound = jnp.max(jnp.sum(jnp.abs(system), axis=1))
        scale = 2.0 / (inflation + bound)
        stack[up] = eye - scale * system
        stack[down] = scale * cross

        def loop(dot):
            def body(carry):
                step, _ = carry
                residue = stack[up]
                size = jnp.sum(residue * residue)
                moved = dot(stack[...], residue, NN)
                stack[down] = stack[down] + moved[members:]
                stack[up] = moved[:members]
                return step + 1, size

            lax.while_loop(lambda c: jnp.logical_and(c[0] < 64, c[1] > 1e-6), body, (jnp.int32(0), jnp.float32(1e9)))

        pl.when(bound <= 300.0)(lambda: loop(dot3))
        pl.when(jnp.logical_not(bound <= 300.0))(lambda: loop(dot_exact))
        return stack[down]

    gram0 = sums[0]
    change = solve(gram0, sums[1] - gram0)
    change = change - jnp.mean(change, axis=1, keepdims=True)
    result[...] = change
    for i in range(1, ITERS):
        change = result[...]
        dev_op[...] = eye + change - jnp.mean(eye + change, axis=0, keepdims=True)
        stack[up] = sums[0] + dot3(change, sums[0], NN)
        stack[down] = sums[1 + i]
        both = dot3(stack[...], dev_op[...], NT)
        v = both[:members]
        z = solve(v - jnp.mean(v, axis=0, keepdims=True), both[members:] - v)
        result[...] = result[...] + dot3(z, dev_op[...], NN)


def final_kernel(n_cell, change, prior, block, weights, *refs):
    others, (posterior, post_predicted) = refs[:n_cell - 1], refs[n_cell - 1:]
    cell = lax.axis_index("cell")
    nblocks = prior.shape[1] // BLK
    fields = [(prior, cell * nblocks)]
    fields += [(other, lax.rem(cell + d + 1, n_cell) * nblocks) for d, other in enumerate(others)]
    predicted = block_predictions(fields, weights, block[...])
    field = prior[...].astype(jnp.float32)
    shift = change[...]
    field_dev = field - jnp.mean(field, axis=0, keepdims=True)
    posterior[...] = (field + dot3(shift, field_dev, NN)).astype(jnp.bfloat16)
    pred_dev = predicted - jnp.mean(predicted, axis=0, keepdims=True)
    post_predicted[...] = predicted + dot3(shift, pred_dev, NN)


def per_device(n_cell, n_obs, prior, obs_block, obs_weight, observed, obs_sigma, pert_seed):
    members, width = prior.shape
    count = obs_block.shape[0]
    block, observed, sigma = (x.reshape(1, count) for x in (obs_block, observed, obs_sigma))
    wide = prior.astype(jnp.float32)
    others = []
    for d in range(1, n_cell):
        others.append(lax.ppermute(wide, "cell", [((i + d) % n_cell, i) for i in range(n_cell)]))
    unit = 8 * n_cell * n_obs
    rows = -(-2 * members // unit) * unit
    lanes = -(-members // 128) * 128
    quarter = rows // n_obs
    stages = 2 * (n_obs.bit_length() - 1) + 2
    f32 = jnp.float32
    sums = pl.pallas_call(
        functools.partial(sums_kernel, n_cell, n_obs),
        out_shape=jax.ShapeDtypeStruct((4, members, members), f32),
        in_specs=[VM] * 6,
        out_specs=VM,
        scratch_shapes=[
            pltpu.VMEM((2, rows, lanes), f32),
            pltpu.VMEM((2, rows, lanes), f32),
            pltpu.VMEM((2, rows, lanes), f32),
            pltpu.VMEM((2, n_cell - 1, quarter // n_cell, lanes), f32),
            pltpu.SemaphoreType.DMA((2, stages, n_cell - 1)),
            pltpu.SemaphoreType.DMA((2, stages, n_cell - 1)),
        ],
        compiler_params=pltpu.CompilerParams(collective_id=0, has_side_effects=True, vmem_limit_bytes=48 << 20),
        cost_estimate=pl.CostEstimate(flops=2_000_000_000, bytes_accessed=4_000_000, transcendentals=0),
        name="sums",
    )(prior, block, obs_weight, observed, sigma, pert_seed)
    change = pl.pallas_call(
        solve_kernel,
        out_shape=jax.ShapeDtypeStruct((members, members), f32),
        in_specs=[VM],
        out_specs=VM,
        scratch_shapes=[pltpu.VMEM((2 * members, members), f32), pltpu.VMEM((members, members), f32)],
        cost_estimate=pl.CostEstimate(flops=20_000_000_000, bytes_accessed=60_000_000, transcendentals=0),
        name="solve",
    )(sums)
    return pl.pallas_call(
        functools.partial(final_kernel, n_cell),
        out_shape=(jax.ShapeDtypeStruct((members, width), jnp.bfloat16),
                   jax.ShapeDtypeStruct((members, count), f32)),
        in_specs=[VM] * (4 + len(others)),
        out_specs=(VM, VM),
        name="final",
    )(change, prior, block, obs_weight, *others)


def solution(mesh):
    return jax.shard_map(
        functools.partial(per_device, mesh.shape["cell"], mesh.shape["obs"]),
        mesh=mesh,
        in_specs=(
            P("scen", "cell"),
            P("obs"),
            P("obs", None),
            P(("scen", "obs")),
            P("obs"),
            P("scen", None, "obs"),
        ),
        out_specs=(P("scen", "cell"), P("scen", "obs")),
        check_vma=False,
    )
```

```python
import functools

import jax
import jax.numpy as jnp
from jax import lax
from jax.experimental import pallas as pl
from jax.experimental.pallas import tpu as pltpu
from jax.sharding import PartitionSpec as P

BLK = 128
ITERS = 3
MESH = pl.DeviceIdType.MESH
VM = pl.BlockSpec(memory_space=pltpu.VMEM)
NN = (((1,), (0,)), ((), ()))
NT = (((1,), (1,)), ((), ()))


def mm(a, b, dims):
    return lax.dot_general(a, b, dims, preferred_element_type=jnp.float32)


def split(x):
    hi = x.astype(jnp.bfloat16)
    return hi, (x - hi.astype(jnp.float32)).astype(jnp.bfloat16)


def dot3(a, b, dims):
    ah, al = split(a)
    bh, bl = split(b)
    return mm(ah, bh, dims) + (mm(ah, bl, dims) + mm(al, bh, dims))


def dot_exact(a, b, dims):
    return lax.dot_general(a, b, dims, precision=lax.Precision.HIGHEST, preferred_element_type=jnp.float32)


def block_predictions(fields, weights, block):
    total = None
    for field, first in fields:
        for b in range(field.shape[1] // BLK):
            part = mm(field[:, b * BLK:(b + 1) * BLK].astype(jnp.bfloat16), weights[...], NT)
            here = block == first + b
            total = jnp.where(here, part, 0.0 if total is None else total)
    return total


def sums_kernel(n_cell, n_obs, sizes, prior_in, block_in, weights_in, observed_in, sigma_in, seeds_in, out, pred,
                prior, block, weights, observed, sigma, seeds, acc, fin, obs_recv, cell_recv, own, gath,
                load_sem, send_sem, recv_sem, gsend_sem, grecv_sem):
    loads = [
        pltpu.make_async_copy(a, b, load_sem.at[i])
        for i, (a, b) in enumerate(((prior_in, prior), (weights_in, weights), (block_in, block), (sigma_in, sigma),
                                    (observed_in, observed), (seeds_in, seeds)))
    ]
    for load in loads:
        load.start()
    members, width = prior.shape
    cell, obs = lax.axis_index("cell"), lax.axis_index("obs")
    bits = [1 << k for k in range(n_obs.bit_length() - 1)]
    barrier = pltpu.get_barrier_semaphore()
    for bit in bits:
        pl.semaphore_signal(barrier, inc=1, device_id={"obs": obs ^ bit}, device_id_type=MESH)
    for d in range(1, n_cell):
        pl.semaphore_signal(barrier, inc=1, device_id={"cell": lax.rem(cell + d, n_cell)}, device_id_type=MESH)

    nblocks = width // BLK
    first = cell * nblocks
    pieces, piece = gath.shape[0], gath.shape[3]
    part = obs & (pieces - 1)
    gbits = [pieces >> (k + 1) for k in range(pieces.bit_length() - 1)]
    held = [0]
    gflights = []

    def remote(src, dst, send, recv, to):
        return pltpu.make_async_remote_copy(src_ref=src, dst_ref=dst, send_sem=send, recv_sem=recv, device_id=to,
                                            device_id_type=MESH)

    def add_blocks(slots):
        blk = block[...]
        for slot in slots:
            for d in range(1, n_cell):
                source = lax.rem(cell + n_cell - d, n_cell) * nblocks + slot * (piece // BLK)
                for b in range(piece // BLK):
                    field = gath[slot, d - 1, :, b * BLK:(b + 1) * BLK].astype(jnp.bfloat16)
                    pred[...] = jnp.where(blk == source + b, mm(field, weights[...], NT), pred[...])

    def gather_start(g):
        if g == 0:
            for d in range(1, n_cell):
                gflights.append(remote(own, gath.at[part, d - 1], gsend_sem.at[g, d - 1], grecv_sem.at[g, d - 1],
                                       {"cell": lax.rem(cell + d, n_cell)}))
        else:
            for j, h in enumerate(held):
                gflights.append(remote(gath.at[part ^ h], gath.at[part ^ h], gsend_sem.at[g, j], grecv_sem.at[g, j],
                                       {"obs": obs ^ gbits[g - 1]}))
        for c in gflights:
            c.start()

    def gather_step(g):
        for c in gflights:
            c.wait()
        gflights.clear()
        fresh = [0] if g == 0 else [h ^ gbits[g - 1] for h in held]
        if g > 0:
            held.extend(fresh)
        if g < len(gbits):
            gather_start(g + 1)
        add_blocks([part ^ h for h in fresh])

    loads[0].wait()
    own[...] = prior[:, pl.ds(pl.multiple_of(part * piece, BLK), piece)].astype(jnp.float32)
    for load in loads[1:]:
        load.wait()
    blk = block[...]
    predicted = block_predictions([(prior, first)], weights, blk)
    pl.semaphore_wait(barrier, len(bits) + n_cell - 1)
    gather_start(0)
    pred[...] = predicted
    inside = jnp.logical_and(blk >= first, blk < first + nblocks)
    mean = jnp.mean(predicted, axis=0, keepdims=True)
    inv = 1.0 / sigma[...]
    dev = (predicted - mean) * jnp.where(inside, inv, 0.0)
    base = (observed[...] - mean) * inv + (3.0 / 1048576.0 - 3.0)
    ah, al = split(dev)
    scale = 1.0 / (members - 1.0)

    def put(k):
        if k == 0:
            h, l = ah, al
        else:
            h, l = split(base + seeds[k - 1].astype(jnp.float32) * (6.0 / 1048576.0))
        acc[k * members:(k + 1) * members, 0:members] = (mm(h, ah, NT) + (mm(h, al, NT) + mm(l, ah, NT))) * scale

    nbit = len(bits)
    bases = [sum(sizes[:s]) for s in range(len(sizes))]
    lens = [[size >> k for k in range(nbit + 1)] for size in sizes]
    offs = []
    for s, base_row in enumerate(bases):
        at = [jnp.int32(base_row)]
        for k in range(nbit):
            at.append(pl.multiple_of(at[-1] + ((obs >> k) & 1) * lens[s][k + 1], 8))
        offs.append(at)
    stages = 2 * nbit + 2

    def copies(s, stage):
        made = []
        chunk = lens[s][-1] // n_cell
        if stage < nbit:
            n = lens[s][stage + 1]
            src = pl.multiple_of(offs[s][stage] + (1 - ((obs >> stage) & 1)) * n, 8)
            made.append((acc.at[pl.ds(src, n)], obs_recv.at[pl.ds(bases[s] + sizes[s] - 2 * n, n)], {"obs": obs ^ bits[stage]}))
        elif stage == nbit:
            for d in range(1, n_cell):
                to = lax.rem(cell + d, n_cell)
                src = pl.multiple_of(offs[s][-1] + to * chunk, 8)
                made.append((acc.at[pl.ds(src, chunk)], cell_recv.at[s, d - 1, pl.ds(0, chunk)], {"cell": to}))
        elif stage == nbit + 1:
            mine = pl.ds(pl.multiple_of(offs[s][-1] + cell * chunk, 8), chunk)
            for d in range(1, n_cell):
                made.append((fin.at[mine], fin.at[mine], {"cell": lax.rem(cell + d, n_cell)}))
        else:
            k = stages - 1 - stage
            mine = pl.ds(offs[s][k + 1], lens[s][k + 1])
            made.append((fin.at[mine], fin.at[mine], {"obs": obs ^ bits[k]}))
        return [remote(a, b, send_sem.at[s, stage, j], recv_sem.at[s, stage, j], to) for j, (a, b, to) in enumerate(made)]

    flights = {}

    def start(s, stage):
        flights[s, stage] = copies(s, stage)
        for c in flights[s, stage]:
            c.start()

    def finish(s, stage):
        for c in flights[s, stage]:
            c.wait()
        if stage < nbit:
            n = lens[s][stage + 1]
            mine = pl.ds(offs[s][stage + 1], n)
            acc[mine] = acc[mine] + obs_recv[pl.ds(bases[s] + sizes[s] - 2 * n, n)]
        elif stage == nbit:
            chunk = lens[s][-1] // n_cell
            mine = pl.ds(pl.multiple_of(offs[s][-1] + cell * chunk, 8), chunk)
            total = acc[mine]
            for d in range(1, n_cell):
                total = total + cell_recv[s, d - 1, pl.ds(0, chunk)]
            fin[mine] = total

    acc[...] = jnp.zeros_like(acc)
    done = 0
    for s in range(len(sizes)):
        while done < ITERS + 1 and done * members < bases[s] + sizes[s]:
            put(done)
            done += 1
        if s == 0:
            start(0, 0)
    second = len(sizes) > 1
    gathers = 0
    for stage in range(stages + 1):
        if stage < stages:
            finish(0, stage)
            if stage + 1 < stages:
                start(0, stage + 1)
        if second:
            if stage > 0:
                finish(1, stage - 1)
            if stage < stages:
                start(1, stage)
        if stage % 2 == 1 and gathers <= len(gbits):
            gather_step(gathers)
            gathers += 1
    while gathers <= len(gbits):
        gather_step(gathers)
        gathers += 1
    for k in range(ITERS + 1):
        out[k] = fin[k * members:(k + 1) * members, 0:members]


def solve_kernel(sums_in, prior_in, predicted_in, posterior, post_predicted, sums, prior, predicted, result, stack,
                 dev_op, load_sem):
    loads = [
        pltpu.make_async_copy(a, b, load_sem.at[i])
        for i, (a, b) in enumerate(((sums_in, sums), (prior_in, prior), (predicted_in, predicted)))
    ]
    for load in loads:
        load.start()
    loads[0].wait()
    members = result.shape[0]
    row = lax.broadcasted_iota(jnp.int32, (members, members), 0)
    col = lax.broadcasted_iota(jnp.int32, (members, members), 1)
    eye = jnp.where(row == col, 1.0, 0.0)
    inflation = float(ITERS)
    up, down = pl.ds(0, members), pl.ds(members, members)

    def solve(gram, cross):
        system = gram + inflation * eye
        bound = jnp.max(jnp.sum(jnp.abs(system), axis=1))
        scale = 2.0 / (inflation + bound)
        stack[up] = eye - scale * system
        stack[down] = scale * cross

        def loop(dot):
            def body(carry):
                step, _ = carry
                residue = stack[up]
                size = jnp.sum(residue * residue)
                moved = dot(stack[...], residue, NN)
                stack[down] = stack[down] + moved[members:]
                stack[up] = moved[:members]
                return step + 1, size

            lax.while_loop(lambda c: jnp.logical_and(c[0] < 64, c[1] > 1e-6), body, (jnp.int32(0), jnp.float32(1e9)))

        pl.when(bound <= 300.0)(lambda: loop(dot3))
        pl.when(jnp.logical_not(bound <= 300.0))(lambda: loop(dot_exact))
        return stack[down]

    gram0 = sums[0]
    change = solve(gram0, sums[1] - gram0)
    change = change - jnp.mean(change, axis=1, keepdims=True)
    result[...] = change
    for i in range(1, ITERS):
        change = result[...]
        dev_op[...] = eye + change - jnp.mean(eye + change, axis=0, keepdims=True)
        stack[up] = sums[0] + dot3(change, sums[0], NN)
        stack[down] = sums[1 + i]
        both = dot3(stack[...], dev_op[...], NT)
        v = both[:members]
        z = solve(v - jnp.mean(v, axis=0, keepdims=True), both[members:] - v)
        result[...] = result[...] + dot3(z, dev_op[...], NN)
    shift = result[...]
    for load in loads[1:]:
        load.wait()
    field = prior[...].astype(jnp.float32)
    field_dev = field - jnp.mean(field, axis=0, keepdims=True)
    posterior[...] = (field + dot3(shift, field_dev, NN)).astype(jnp.bfloat16)
    first = predicted[...]
    post_predicted[...] = first + dot3(shift, first - jnp.mean(first, axis=0, keepdims=True), NN)


def per_device(n_cell, n_obs, prior, obs_block, obs_weight, observed, obs_sigma, pert_seed):
    members, width = prior.shape
    count = obs_block.shape[0]
    block, observed, sigma = (x.reshape(1, count) for x in (obs_block, observed, obs_sigma))
    unit = 8 * n_cell * n_obs
    units = -(-(ITERS + 1) * members // unit)
    sizes = [unit * (units - units // 2), unit * (units // 2)] if units > 1 else [unit]
    rows = sum(sizes)
    lanes = -(-members // 128) * 128
    stages = 2 * (n_obs.bit_length() - 1) + 2
    pieces = min(n_obs, width // BLK)
    piece = width // pieces
    f32 = jnp.float32
    hbm = pl.BlockSpec(memory_space=pltpu.HBM)
    gstages = pieces.bit_length()
    gcopies = max(n_cell - 1, pieces)
    sums, predicted = pl.pallas_call(
        functools.partial(sums_kernel, n_cell, n_obs, sizes),
        out_shape=(jax.ShapeDtypeStruct((ITERS + 1, members, members), f32),
                   jax.ShapeDtypeStruct((members, count), f32)),
        in_specs=[hbm] * 6,
        out_specs=(VM, VM),
        scratch_shapes=[
            pltpu.VMEM(prior.shape, prior.dtype),
            pltpu.VMEM(block.shape, block.dtype),
            pltpu.VMEM(obs_weight.shape, obs_weight.dtype),
            pltpu.VMEM(observed.shape, f32),
            pltpu.VMEM(sigma.shape, f32),
            pltpu.VMEM(pert_seed.shape, pert_seed.dtype),
            pltpu.VMEM((rows, lanes), f32),
            pltpu.VMEM((rows, lanes), f32),
            pltpu.VMEM((rows, lanes), f32),
            pltpu.VMEM((len(sizes), n_cell - 1, sizes[0] // n_obs // n_cell, lanes), f32),
            pltpu.VMEM((members, piece), f32),
            pltpu.VMEM((pieces, n_cell - 1, members, piece), f32),
            pltpu.SemaphoreType.DMA((6,)),
            pltpu.SemaphoreType.DMA((len(sizes), stages, n_cell - 1)),
            pltpu.SemaphoreType.DMA((len(sizes), stages, n_cell - 1)),
            pltpu.SemaphoreType.DMA((gstages, gcopies)),
            pltpu.SemaphoreType.DMA((gstages, gcopies)),
        ],
        compiler_params=pltpu.CompilerParams(collective_id=0, has_side_effects=True, vmem_limit_bytes=67043328),
        name="sums",
    )(prior, block, obs_weight, observed, sigma, pert_seed)
    return pl.pallas_call(
        solve_kernel,
        out_shape=(jax.ShapeDtypeStruct((members, width), jnp.bfloat16),
                   jax.ShapeDtypeStruct((members, count), f32)),
        in_specs=[hbm] * 3,
        out_specs=(VM, VM),
        scratch_shapes=[
            pltpu.VMEM(sums.shape, f32),
            pltpu.VMEM(prior.shape, prior.dtype),
            pltpu.VMEM(predicted.shape, f32),
            pltpu.VMEM((members, members), f32),
            pltpu.VMEM((2 * members, members), f32),
            pltpu.VMEM((members, members), f32),
            pltpu.SemaphoreType.DMA((3,)),
        ],
        compiler_params=pltpu.CompilerParams(vmem_limit_bytes=67043328),
        name="solve",
    )(sums, prior, predicted)


def solution(mesh):
    return jax.shard_map(
        functools.partial(per_device, mesh.shape["cell"], mesh.shape["obs"]),
        mesh=mesh,
        in_specs=(
            P("scen", "cell"),
            P("obs"),
            P("obs", None),
            P(("scen", "obs")),
            P("obs"),
            P("scen", None, "obs"),
        ),
        out_specs=(P("scen", "cell"), P("scen", "obs")),
        check_vma=False,
    )
```

```python
import functools

import jax
import jax.numpy as jnp
from jax import lax
from jax.experimental import pallas as pl
from jax.experimental.pallas import tpu as pltpu
from jax.sharding import PartitionSpec as P

BLK = 128
ITERS = 3
MESH = pl.DeviceIdType.MESH
VM = pl.BlockSpec(memory_space=pltpu.VMEM)
NN = (((1,), (0,)), ((), ()))
NT = (((1,), (1,)), ((), ()))


def mm(a, b, dims):
    return lax.dot_general(a, b, dims, preferred_element_type=jnp.float32)


def split(x):
    hi = x.astype(jnp.bfloat16)
    return hi, (x - hi.astype(jnp.float32)).astype(jnp.bfloat16)


def dot3(a, b, dims):
    ah, al = split(a)
    bh, bl = split(b)
    return mm(ah, bh, dims) + (mm(ah, bl, dims) + mm(al, bh, dims))


def dot_exact(a, b, dims):
    return lax.dot_general(a, b, dims, precision=lax.Precision.HIGHEST, preferred_element_type=jnp.float32)


def block_predictions(fields, weights, block):
    total = None
    for field, first in fields:
        for b in range(field.shape[1] // BLK):
            part = mm(field[:, b * BLK:(b + 1) * BLK].astype(jnp.bfloat16), weights[...], NT)
            here = block == first + b
            total = jnp.where(here, part, 0.0 if total is None else total)
    return total


def sums_kernel(n_cell, n_obs, sizes, prior_in, block_in, weights_in, observed_in, sigma_in, seeds_in, out, pred,
                prior, block, weights, observed, sigma, seeds, acc, fin, obs_recv, cell_recv, own, gath,
                load_sem, send_sem, recv_sem, gsend_sem, grecv_sem):
    loads = [
        pltpu.make_async_copy(a, b, load_sem.at[i])
        for i, (a, b) in enumerate(((prior_in, prior), (weights_in, weights), (block_in, block), (sigma_in, sigma),
                                    (observed_in, observed), (seeds_in, seeds)))
    ]
    for load in loads:
        load.start()
    members, width = prior.shape
    cell, obs = lax.axis_index("cell"), lax.axis_index("obs")
    bits = [1 << k for k in range(n_obs.bit_length() - 1)]
    barrier = pltpu.get_barrier_semaphore()
    for bit in bits:
        pl.semaphore_signal(barrier, inc=1, device_id={"obs": obs ^ bit}, device_id_type=MESH)
    for d in range(1, n_cell):
        pl.semaphore_signal(barrier, inc=1, device_id={"cell": lax.rem(cell + d, n_cell)}, device_id_type=MESH)

    nblocks = width // BLK
    first = cell * nblocks
    pieces, piece = gath.shape[0], gath.shape[3]
    part = obs & (pieces - 1)
    gbits = [pieces >> (k + 1) for k in range(pieces.bit_length() - 1)]
    held = [0]
    gflights = []

    def remote(src, dst, send, recv, to):
        return pltpu.make_async_remote_copy(src_ref=src, dst_ref=dst, send_sem=send, recv_sem=recv, device_id=to,
                                            device_id_type=MESH)

    def add_blocks(slots):
        blk = block[...]
        for slot in slots:
            for d in range(1, n_cell):
                source = lax.rem(cell + n_cell - d, n_cell) * nblocks + slot * (piece // BLK)
                for b in range(piece // BLK):
                    field = gath[slot, d - 1, :, b * BLK:(b + 1) * BLK].astype(jnp.bfloat16)
                    pred[...] = jnp.where(blk == source + b, mm(field, weights[...], NT), pred[...])

    def gather_start(g):
        if g == 0:
            for d in range(1, n_cell):
                gflights.append(remote(own, gath.at[part, d - 1], gsend_sem.at[g, d - 1], grecv_sem.at[g, d - 1],
                                       {"cell": lax.rem(cell + d, n_cell)}))
        else:
            for j, h in enumerate(held):
                gflights.append(remote(gath.at[part ^ h], gath.at[part ^ h], gsend_sem.at[g, j], grecv_sem.at[g, j],
                                       {"obs": obs ^ gbits[g - 1]}))
        for c in gflights:
            c.start()

    def gather_step(g):
        for c in gflights:
            c.wait()
        gflights.clear()
        fresh = [0] if g == 0 else [h ^ gbits[g - 1] for h in held]
        if g > 0:
            held.extend(fresh)
        if g < len(gbits):
            gather_start(g + 1)
        add_blocks([part ^ h for h in fresh])

    loads[0].wait()
    own[...] = prior[:, pl.ds(pl.multiple_of(part * piece, BLK), piece)].astype(jnp.float32)
    for load in loads[1:5]:
        load.wait()
    blk = block[...]
    predicted = block_predictions([(prior, first)], weights, blk)
    pl.semaphore_wait(barrier, len(bits) + n_cell - 1)
    gather_start(0)
    pred[...] = predicted
    inside = jnp.logical_and(blk >= first, blk < first + nblocks)
    mean = jnp.mean(predicted, axis=0, keepdims=True)
    inv = 1.0 / sigma[...]
    dev = (predicted - mean) * jnp.where(inside, inv, 0.0)
    base = (observed[...] - mean) * inv + (3.0 / 1048576.0 - 3.0)
    ah, al = split(dev)
    scale = 1.0 / (members - 1.0)

    def put(k):
        if k == 0:
            h, l = ah, al
        else:
            h, l = split(base + seeds[k - 1].astype(jnp.float32) * (6.0 / 1048576.0))
        acc[k * members:(k + 1) * members, 0:members] = (mm(h, ah, NT) + (mm(h, al, NT) + mm(l, ah, NT))) * scale

    nbit = len(bits)
    bases = [sum(sizes[:s]) for s in range(len(sizes))]
    lens = [[size >> k for k in range(nbit + 1)] for size in sizes]
    offs = []
    for s, base_row in enumerate(bases):
        at = [jnp.int32(base_row)]
        for k in range(nbit):
            at.append(pl.multiple_of(at[-1] + ((obs >> k) & 1) * lens[s][k + 1], 8))
        offs.append(at)
    stages = 2 * nbit + 2

    def copies(s, stage):
        made = []
        chunk = lens[s][-1] // n_cell
        if stage < nbit:
            n = lens[s][stage + 1]
            src = pl.multiple_of(offs[s][stage] + (1 - ((obs >> stage) & 1)) * n, 8)
            made.append((acc.at[pl.ds(src, n)], obs_recv.at[pl.ds(bases[s] + sizes[s] - 2 * n, n)], {"obs": obs ^ bits[stage]}))
        elif stage == nbit:
            for d in range(1, n_cell):
                to = lax.rem(cell + d, n_cell)
                src = pl.multiple_of(offs[s][-1] + to * chunk, 8)
                made.append((acc.at[pl.ds(src, chunk)], cell_recv.at[s, d - 1, pl.ds(0, chunk)], {"cell": to}))
        elif stage == nbit + 1:
            mine = pl.ds(pl.multiple_of(offs[s][-1] + cell * chunk, 8), chunk)
            for d in range(1, n_cell):
                made.append((fin.at[mine], fin.at[mine], {"cell": lax.rem(cell + d, n_cell)}))
        else:
            k = stages - 1 - stage
            mine = pl.ds(offs[s][k + 1], lens[s][k + 1])
            made.append((fin.at[mine], fin.at[mine], {"obs": obs ^ bits[k]}))
        return [remote(a, b, send_sem.at[s, stage, j], recv_sem.at[s, stage, j], to) for j, (a, b, to) in enumerate(made)]

    flights = {}

    def start(s, stage):
        flights[s, stage] = copies(s, stage)
        for c in flights[s, stage]:
            c.start()

    def finish(s, stage):
        for c in flights[s, stage]:
            c.wait()
        if stage < nbit:
            n = lens[s][stage + 1]
            mine = pl.ds(offs[s][stage + 1], n)
            acc[mine] = acc[mine] + obs_recv[pl.ds(bases[s] + sizes[s] - 2 * n, n)]
        elif stage == nbit:
            chunk = lens[s][-1] // n_cell
            mine = pl.ds(pl.multiple_of(offs[s][-1] + cell * chunk, 8), chunk)
            total = acc[mine]
            for d in range(1, n_cell):
                total = total + cell_recv[s, d - 1, pl.ds(0, chunk)]
            fin[mine] = total

    acc[...] = jnp.zeros_like(acc)
    put(0)
    loads[5].wait()
    done, count = 1, len(sizes)
    for s in range(count):
        while done < ITERS + 1 and done * members < bases[s] + sizes[s]:
            put(done)
            done += 1
        start(s, 0)
    gathers = 0
    for step in range(stages + count - 1):
        for s in range(count):
            stage = step - s
            if 0 <= stage < stages:
                finish(s, stage)
                if stage + 1 < stages:
                    start(s, stage + 1)
        if step >= count - 1 and (step - count) % 3 == 2 and gathers <= len(gbits):
            gather_step(gathers)
            gathers += 1
    while gathers <= len(gbits):
        gather_step(gathers)
        gathers += 1
    for k in range(ITERS + 1):
        out[k] = fin[k * members:(k + 1) * members, 0:members]


def solve_kernel(sums_in, prior_in, predicted_in, posterior, post_predicted, sums, prior, predicted, result, stack,
                 dev_op, load_sem):
    loads = [
        pltpu.make_async_copy(a, b, load_sem.at[i])
        for i, (a, b) in enumerate(((sums_in, sums), (prior_in, prior), (predicted_in, predicted)))
    ]
    for load in loads:
        load.start()
    loads[0].wait()
    members = result.shape[0]
    row = lax.broadcasted_iota(jnp.int32, (members, members), 0)
    col = lax.broadcasted_iota(jnp.int32, (members, members), 1)
    eye = jnp.where(row == col, 1.0, 0.0)
    inflation = float(ITERS)
    up, down = pl.ds(0, members), pl.ds(members, members)

    def solve(gram, cross):
        system = gram + inflation * eye
        bound = jnp.max(jnp.sum(jnp.abs(system), axis=1))
        scale = 2.0 / (inflation + bound)
        stack[up] = eye - scale * system
        stack[down] = scale * cross

        def loop(dot):
            def body(carry):
                step, _ = carry
                residue = stack[up]
                size = jnp.sum(residue * residue)
                moved = dot(stack[...], residue, NN)
                stack[down] = stack[down] + moved[members:]
                stack[up] = moved[:members]
                return step + 1, size

            lax.while_loop(lambda c: jnp.logical_and(c[0] < 64, c[1] > 1e-6), body, (jnp.int32(0), jnp.float32(1e9)))

        pl.when(bound <= 300.0)(lambda: loop(dot3))
        pl.when(jnp.logical_not(bound <= 300.0))(lambda: loop(dot_exact))
        return stack[down]

    gram0 = sums[0]
    change = solve(gram0, sums[1] - gram0)
    change = change - jnp.mean(change, axis=1, keepdims=True)
    result[...] = change
    for i in range(1, ITERS):
        change = result[...]
        dev_op[...] = eye + change - jnp.mean(eye + change, axis=0, keepdims=True)
        stack[up] = sums[0] + dot3(change, sums[0], NN)
        stack[down] = sums[1 + i]
        both = dot3(stack[...], dev_op[...], NT)
        v = both[:members]
        z = solve(v - jnp.mean(v, axis=0, keepdims=True), both[members:] - v)
        result[...] = result[...] + dot3(z, dev_op[...], NN)
    shift = result[...]
    for load in loads[1:]:
        load.wait()
    field = prior[...].astype(jnp.float32)
    field_dev = field - jnp.mean(field, axis=0, keepdims=True)
    posterior[...] = (field + dot3(shift, field_dev, NN)).astype(jnp.bfloat16)
    first = predicted[...]
    post_predicted[...] = first + dot3(shift, first - jnp.mean(first, axis=0, keepdims=True), NN)


def per_device(n_cell, n_obs, prior, obs_block, obs_weight, observed, obs_sigma, pert_seed):
    members, width = prior.shape
    count = obs_block.shape[0]
    block, observed, sigma = (x.reshape(1, count) for x in (obs_block, observed, obs_sigma))
    unit = 8 * n_cell * n_obs
    units = -(-(ITERS + 1) * members // unit)
    count_sets = min(3, units)
    sizes = [unit * (units // count_sets + (s < units % count_sets)) for s in range(count_sets)]
    rows = sum(sizes)
    lanes = -(-members // 128) * 128
    stages = 2 * (n_obs.bit_length() - 1) + 2
    pieces = min(n_obs, width // BLK)
    piece = width // pieces
    f32 = jnp.float32
    hbm = pl.BlockSpec(memory_space=pltpu.HBM)
    gstages = pieces.bit_length()
    gcopies = max(n_cell - 1, pieces)
    sums, predicted = pl.pallas_call(
        functools.partial(sums_kernel, n_cell, n_obs, sizes),
        out_shape=(jax.ShapeDtypeStruct((ITERS + 1, members, members), f32),
                   jax.ShapeDtypeStruct((members, count), f32)),
        in_specs=[hbm] * 6,
        out_specs=(VM, VM),
        scratch_shapes=[
            pltpu.VMEM(prior.shape, prior.dtype),
            pltpu.VMEM(block.shape, block.dtype),
            pltpu.VMEM(obs_weight.shape, obs_weight.dtype),
            pltpu.VMEM(observed.shape, f32),
            pltpu.VMEM(sigma.shape, f32),
            pltpu.VMEM(pert_seed.shape, pert_seed.dtype),
            pltpu.VMEM((rows, lanes), f32),
            pltpu.VMEM((rows, lanes), f32),
            pltpu.VMEM((rows, lanes), f32),
            pltpu.VMEM((len(sizes), n_cell - 1, sizes[0] // n_obs // n_cell, lanes), f32),
            pltpu.VMEM((members, piece), f32),
            pltpu.VMEM((pieces, n_cell - 1, members, piece), f32),
            pltpu.SemaphoreType.DMA((6,)),
            pltpu.SemaphoreType.DMA((len(sizes), stages, n_cell - 1)),
            pltpu.SemaphoreType.DMA((len(sizes), stages, n_cell - 1)),
            pltpu.SemaphoreType.DMA((gstages, gcopies)),
            pltpu.SemaphoreType.DMA((gstages, gcopies)),
        ],
        compiler_params=pltpu.CompilerParams(collective_id=0, has_side_effects=True, vmem_limit_bytes=67043328),
        name="sums",
    )(prior, block, obs_weight, observed, sigma, pert_seed)
    return pl.pallas_call(
        solve_kernel,
        out_shape=(jax.ShapeDtypeStruct((members, width), jnp.bfloat16),
                   jax.ShapeDtypeStruct((members, count), f32)),
        in_specs=[hbm] * 3,
        out_specs=(VM, VM),
        scratch_shapes=[
            pltpu.VMEM(sums.shape, f32),
            pltpu.VMEM(prior.shape, prior.dtype),
            pltpu.VMEM(predicted.shape, f32),
            pltpu.VMEM((members, members), f32),
            pltpu.VMEM((2 * members, members), f32),
            pltpu.VMEM((members, members), f32),
            pltpu.SemaphoreType.DMA((3,)),
        ],
        compiler_params=pltpu.CompilerParams(vmem_limit_bytes=67043328),
        name="solve",
    )(sums, prior, predicted)


def solution(mesh):
    return jax.shard_map(
        functools.partial(per_device, mesh.shape["cell"], mesh.shape["obs"]),
        mesh=mesh,
        in_specs=(
            P("scen", "cell"),
            P("obs"),
            P("obs", None),
            P(("scen", "obs")),
            P("obs"),
            P("scen", None, "obs"),
        ),
        out_specs=(P("scen", "cell"), P("scen", "obs")),
        check_vma=False,
    )
```
